768 devices in a mesh: grp: 48 (over z_hi, y, core), tp: 16 (over z_lo, x).
Axes of the slice: x: 4, y: 8, z: 12 (z_hi: 3, z_lo: 4; z = z_hi * 4 + z_lo), core: 2. Of those that a mesh axis runs over, the one named last changes fastest.
Arguments:
- text_embeds: bfloat16 [98304, 8192], P('grp', 'tp'), may hold values from -6 to 6
- image_embeds: bfloat16 [49152, 8192], P(('grp', 'tp')), may hold values from -6 to 6
- image_offsets: int32 [96, 2], P('grp'), may hold values from 0 to 768, as said below
- image_counts: int32 [96], P('grp'), may hold values from 1 to 2
- seq_lengths: int32 [96], P('grp'), may hold values from 513 to 1024
- norm_gain: bfloat16 [8192], P('tp'), may hold values from 0.25 to 1.75
- key_weight: bfloat16 [8192, 512], P('tp'), may hold values from -0.0625 to 0.0625
- key_bias: bfloat16 [512], replicated, may hold values from -3 to 3
- key_cotangent: bfloat16 [98304, 512], P(('grp', 'tp')), may hold values from -0.017944336 to 0.017944336
Outputs:
- key_states: bfloat16 [98304, 512], P(('grp', 'tp'))
- weight_grad: float32 [8192, 512], P('tp')
- bias_grad: float32 [512], replicated
- gain_grad: float32 [8192], P('tp')
The draws below stay inside these ranges and needn't reach their ends.
Inputs may be any that keep to these rules, and one draw needn't show every extreme that they name: `image_offsets`: each sequence's first image_counts slots hold increasing starts of non-intersecting runs of 256 rows that end within its used rows; later slots hold 0.
All inputs are finite; a program needn't handle non-finite values.
Results may differ from the reference program's by a relative error of at most 0.0046.
Values may be sent and summed in bfloat16 or wider, within the bound.
No kernel may reach another device: no remote copies, remote signals or barrier semaphores. Data moves between devices by JAX's collectives and lax.ppermute only.
A program may use at most 32 MiB of HBM per device.

```python
import jax
import jax.numpy as jnp
from jax import lax

D = 8192
PATCH_TOK = 256
MAX_IMG = 2
SEQS = 2
LEN = 1024
KEYS = 512
GROUP_ROWS = 2048
IMG_ROWS = 1024
SEQ_TOTAL = 96
TOKENS = 98304
IMG_TOTAL = 49152
N_GRP = 48


def image_layout(key):
    base = jax.random.fold_in(key, 11)
    first_key, second_key, third_key = jax.random.split(base, 3)
    counts = jax.random.randint(first_key, (SEQ_TOTAL,), 1, MAX_IMG + 1).astype(jnp.int32)
    counts = counts.at[0].set(MAX_IMG)
    lengths = jax.random.randint(second_key, (SEQ_TOTAL,), MAX_IMG * PATCH_TOK + 1, LEN + 1).astype(jnp.int32)
    lengths = lengths.at[1].set(LEN)
    spare = lengths - counts * PATCH_TOK
    slot_ids = jnp.arange(MAX_IMG, dtype=jnp.int32)
    starts = jax.random.randint(third_key, (SEQ_TOTAL, MAX_IMG), 0, spare[:, None] + 1).astype(jnp.int32)
    starts = jnp.where(slot_ids[None, :] < counts[:, None], starts, spare[:, None])
    starts = jnp.sort(starts, axis=1)
    offsets = starts + slot_ids[None, :] * PATCH_TOK
    offsets = jnp.where(slot_ids[None, :] < counts[:, None], offsets, 0).astype(jnp.int32)
    return (offsets, counts, lengths)


def draw_image_offsets(key, part):
    return image_layout(key)[0]


def draw_image_counts(key, part):
    return image_layout(key)[1]


def draw_seq_lengths(key, part):
    return image_layout(key)[2]


def levels(own_key, shape, cuts, low, high):
    factor_of, own = 1.0, jax.random.fold_in(own_key, 6)
    for axis_at, shards_of in cuts:
        heights = jnp.exp(jax.random.uniform(jax.random.fold_in(own, axis_at), (shards_of,), jnp.float32, low / len(cuts), high / len(cuts)))
        factor_of = factor_of * jnp.repeat(heights, shape[axis_at] // shards_of).reshape([-1 if axis == axis_at else 1 for axis in range(len(shape))])
    return factor_of


def scatter_about(own_key, shape, scale, most, cuts=(), kind=jnp.bfloat16):
    level = levels(own_key, shape, cuts, -0.22, 0.18) if cuts else 1.0
    drawn = jax.random.normal(own_key, shape, jnp.float32) * scale * level
    return jnp.minimum(jnp.maximum(drawn, -most), most).astype(kind)


def setup_inputs(seed: int = 0) -> dict:
    keys = jax.random.split(jax.random.key(seed), 10)
    return {
        "text_embeds": scatter_about(keys[0], (TOKENS, D), 1.0, 6.0, ((0, 48), (1, 16))),
        "image_embeds": scatter_about(keys[1], (IMG_TOTAL, D), 1.0, 6.0, ((0, 768),)),
        "image_offsets": draw_image_offsets(jax.random.fold_in(keys[9], 71), 0),
        "image_counts": draw_image_counts(jax.random.fold_in(keys[9], 71), 0),
        "seq_lengths": draw_seq_lengths(jax.random.fold_in(keys[9], 71), 0),
        "norm_gain": jnp.clip(1.0 + 0.15 * jax.random.normal(keys[5], (D,), jnp.float32), 0.25, 1.75).astype(jnp.bfloat16),
        "key_weight": scatter_about(keys[6], (D, KEYS), D ** -0.5, 0.0625, ((0, 16),)),
        "key_bias": scatter_about(keys[7], (KEYS,), 0.5, 3.0),
        "key_cotangent": scatter_about(keys[8], (TOKENS, KEYS), 0.003, 0.017944336, ((0, 768),)),
    }


def place_images(text_rows, image_rows, offsets, counts, lengths):
    total_rows = text_rows.shape[0]
    row_ids = jnp.arange(total_rows, dtype=jnp.int32)
    seq_ids = row_ids // LEN
    position = row_ids % LEN
    seq_hot = (seq_ids[:, None] == jnp.arange(offsets.shape[0], dtype=jnp.int32)[None, :]).astype(jnp.int32)
    row_offsets = lax.optimization_barrier(jnp.sum(seq_hot[:, :, None] * offsets[None, :, :], axis=1))
    row_counts = lax.optimization_barrier(jnp.sum(seq_hot * counts[None, :], axis=1))
    row_lengths = lax.optimization_barrier(jnp.sum(seq_hot * lengths[None, :], axis=1))
    slot_ids = jnp.arange(MAX_IMG, dtype=jnp.int32)
    inside = (slot_ids[None, :] < row_counts[:, None]) & (position[:, None] >= row_offsets) & (position[:, None] < row_offsets + PATCH_TOK)
    inside_int = inside.astype(jnp.int32)
    any_inside = lax.optimization_barrier(jnp.sum(inside_int, axis=1)) > 0
    chosen_slot = lax.optimization_barrier(jnp.sum(inside_int * slot_ids[None, :], axis=1))
    chosen_start = lax.optimization_barrier(jnp.sum(inside_int * row_offsets, axis=1))
    source = (seq_ids * MAX_IMG + chosen_slot) * PATCH_TOK + position - chosen_start
    source = jnp.where(any_inside, source, 0).astype(jnp.int32)
    picked = jnp.take(image_rows, source, axis=0)
    merged = jnp.where(any_inside[:, None], picked, text_rows)
    row_valid = (position < row_lengths).astype(jnp.float32)
    return (merged, row_valid)

def reference(text_embeds, image_embeds, image_offsets, image_counts, seq_lengths, norm_gain, key_weight, key_bias, key_cotangent):
    text_groups = text_embeds.reshape(N_GRP, GROUP_ROWS, D)
    image_groups = image_embeds.reshape(N_GRP, IMG_ROWS, D)
    offset_groups = image_offsets.reshape(N_GRP, SEQS, MAX_IMG)
    count_groups = image_counts.reshape(N_GRP, SEQS)
    length_groups = seq_lengths.reshape(N_GRP, SEQS)
    grad_groups = key_cotangent.reshape(N_GRP, GROUP_ROWS, KEYS)
    gain32 = norm_gain.astype(jnp.float32)
    bias32 = key_bias.astype(jnp.float32)

    def one_group(totals, inputs):
        text_rows, image_rows, offsets, counts, lengths, cot_rows = inputs
        merged, row_valid = place_images(text_rows, image_rows, offsets, counts, lengths)
        merged32 = merged.astype(jnp.float32)
        rstd = lax.rsqrt(lax.optimization_barrier(jnp.mean(merged32 * merged32, axis=1)) + 1e-06)
        normed = (merged32 * rstd[:, None] * gain32[None, :]).astype(jnp.bfloat16)
        projected = jnp.dot(normed, key_weight, preferred_element_type=jnp.float32)
        keys_here = ((projected + bias32[None, :]) * row_valid[:, None]).astype(jnp.bfloat16)
        masked_grad = (cot_rows.astype(jnp.float32) * row_valid[:, None]).astype(jnp.bfloat16)
        weight_part = lax.dot_general(normed, masked_grad, (((0,), (0,)), ((), ())), preferred_element_type=jnp.float32)
        bias_part = lax.optimization_barrier(jnp.sum(masked_grad.astype(jnp.float32), axis=0))
        grad_normed = lax.dot_general(masked_grad, key_weight, (((1,), (1,)), ((), ())), preferred_element_type=jnp.float32)
        gain_part = lax.optimization_barrier(jnp.sum(grad_normed * merged32 * rstd[:, None], axis=0))
        return ((totals[0] + weight_part, totals[1] + bias_part, totals[2] + gain_part), keys_here)
    start_totals = (jnp.zeros((D, KEYS), jnp.float32), jnp.zeros((KEYS,), jnp.float32), jnp.zeros((D,), jnp.float32))
    totals, key_groups = lax.scan(one_group, start_totals, (text_groups, image_groups, offset_groups, count_groups, length_groups, grad_groups))
    return (key_groups.reshape(TOKENS, KEYS), totals[0], totals[1], totals[2])
```

```python
import jax
import jax.numpy as jnp
from jax import lax
from jax.experimental import pallas as pl
from jax.experimental.pallas import tpu as pltpu
from jax.sharding import Mesh
from jax.sharding import PartitionSpec as P

D = 8192
PATCH = 256
LEN = 1024
EPS = 1e-06
BF = jnp.bfloat16
F32 = jnp.float32
AXES = ("zh", "y", "c", "zl", "x")
SIZES = (3, 8, 2, 4, 4)
GRP = ("zh", "y", "c")
TP = ("zl", "x")
RING = ("zh", "y")
PIECES = 24
SLAB = 48
HALF = PIECES * SLAB
MIB = 1024 * 1024


def call(kernel, outs, args, smem=0, scratch=(), flops=0, nbytes=0, mib=12):
    in_specs = [pl.BlockSpec(memory_space=pltpu.SMEM)] * smem
    in_specs += [pl.BlockSpec(memory_space=pltpu.VMEM)] * (len(args) - smem)
    many = isinstance(outs, (list, tuple))
    vmem = pl.BlockSpec(memory_space=pltpu.VMEM)
    return pl.pallas_call(
        kernel,
        out_shape=outs,
        in_specs=in_specs,
        out_specs=[vmem] * len(outs) if many else vmem,
        scratch_shapes=list(scratch),
        cost_estimate=pl.CostEstimate(flops=flops, bytes_accessed=nbytes, transcendentals=0),
        compiler_params=pltpu.CompilerParams(vmem_limit_bytes=mib * MIB),
    )(*args)


def shape(dims, dtype):
    return jax.ShapeDtypeStruct(dims, dtype)


def own_valid(length_ref, rows, lanes):
    zl, x = lax.axis_index("zl"), lax.axis_index("x")
    position = (zl % 2) * 512 + x * 128 + lax.broadcasted_iota(jnp.int32, (rows, lanes), 0)
    return (position < length_ref[zl // 2]).astype(F32)


def mask_kernel(length_ref, cot_ref, out_ref):
    out_ref[...] = (cot_ref[...].astype(F32) * own_valid(length_ref, 128, 512)).astype(BF)


def prep_kernel(text_ref, image_ref, out_ref):
    rows = image_ref.shape[0]
    total = jnp.zeros((rows, 512), F32)
    for t in range(16):
        part = image_ref[:, t * 512 : (t + 1) * 512].astype(F32)
        total = total + part * part
    rstd = lax.rsqrt(jnp.sum(total, axis=1, keepdims=True) / D + EPS)
    row = lax.broadcasted_iota(jnp.int32, (8, 512), 0)
    ones = jnp.ones((8, 128), F32)
    parts = jnp.zeros((8, 512), F32)
    for j in range(4):
        lanes = jnp.zeros((512, 128), F32)
        for b in range(4):
            part = text_ref[j * 512 : (j + 1) * 512, b * 128 : (b + 1) * 128].astype(F32)
            lanes = lanes + part * part
        sums = lax.dot_general(
            ones, lanes, (((1,), (1,)), ((), ())), precision=lax.Precision.HIGHEST,
            preferred_element_type=F32,
        )
        top = sums.astype(BF).astype(F32)
        parts = parts + jnp.where(row == j, top, 0.0) + jnp.where(row == j + 4, sums - top, 0.0)
    parts = parts.astype(BF)
    for t in range(16):
        part = image_ref[:, t * 512 : (t + 1) * 512].astype(F32)
        out_ref[t, :64, :] = (part * rstd).astype(BF)
        out_ref[t, 64:, :] = parts


def block(z, q):
    return pl.ds(pl.multiple_of((z * 4 + q) * 128, 128), 128)


def norm_kernel(
    offset_ref, count_ref, text_ref, got_ref, weight_ref, gain_ref, normed_ref, key0_ref, key1_ref, key2_ref, key3_ref
):
    squares = jnp.concatenate([got_ref[t, 64:, :] for t in range(16)], axis=0)
    pick = lax.broadcasted_iota(jnp.int32, (128, 128), 0) % 4
    gain = gain_ref[...].astype(F32)
    for seq in range(2):
        images = jnp.concatenate([got_ref[seq * 8 + t, :64, :] for t in range(8)], axis=0)
        for part in range(4):
            base = part * 256
            ones = (pick == seq * 2 + part // 2).astype(F32).astype(BF)
            cols = slice((part % 2) * 256, (part % 2) * 256 + 256)
            total = lax.dot_general(
                squares[:, cols], ones, (((0,), (0,)), ((), ())), preferred_element_type=F32
            )
            position = base + lax.broadcasted_iota(jnp.int32, (256, 256), 0)
            column = lax.broadcasted_iota(jnp.int32, (256, 256), 1)
            narrow = base + lax.broadcasted_iota(jnp.int32, (256, 128), 0)
            hot, covered = [], None
            for slot in range(2):
                start = jnp.where(slot < count_ref[seq], offset_ref[seq, slot], LEN)
                hot.append((position - start == column).astype(F32).astype(BF))
                here = (narrow >= start) & (narrow < start + PATCH)
                covered = here if covered is None else covered | here
            scale = jnp.where(covered, 1.0, lax.rsqrt(total / D + EPS))
            placed = jnp.dot(hot[0], images[:256], preferred_element_type=F32)
            placed = placed + jnp.dot(hot[1], images[256:], preferred_element_type=F32)
            rows = slice(seq * LEN + base, seq * LEN + base + 256)
            for b in range(4):
                cols = slice(b * 128, (b + 1) * 128)
                text = text_ref[rows, cols].astype(F32)
                value = jnp.where(covered, placed[:, cols], text) * scale * gain[:, cols]
                normed_ref[rows, cols] = value.astype(BF)
    x = lax.axis_index("x")
    for s, key_ref in enumerate((key0_ref, key1_ref, key2_ref, key3_ref)):
        q = lax.rem(x + s, 4)
        normed = jnp.concatenate([normed_ref[block(z, q), :] for z in range(4)], axis=0)
        product = jnp.dot(normed, weight_ref[...], preferred_element_type=F32)
        key_ref[...] = product.astype(key_ref.dtype)


def grad_kernel(normed_ref, own_ref, got1_ref, got2_ref, got3_ref, mine_ref, other_ref, grad_ref):
    x, zl, core = lax.axis_index("x"), lax.axis_index("zl"), lax.axis_index("c")
    bias = jnp.zeros((8, 512), F32)
    for s, source in enumerate((own_ref, got1_ref, got2_ref, got3_ref)):
        q = lax.rem(x - s + 4, 4)
        normed = jnp.concatenate([normed_ref[block(lax.rem(zl - i + 4, 4), q), :] for i in range(4)], axis=0)
        masked = source[...]
        part = lax.dot_general(normed, masked, (((0,), (0,)), ((), ())), preferred_element_type=F32)
        grad_ref[...] = part if s == 0 else grad_ref[...] + part
        bias = bias + jnp.dot(jnp.ones((8, 512), BF), masked, preferred_element_type=F32)
    near = pl.ds(pl.multiple_of(core * 256, 256), 256)
    far = pl.ds(pl.multiple_of((1 - core) * 256, 256), 256)
    for b in range(4):
        cols = slice(b * 128, (b + 1) * 128)
        mine_ref[b * 256 : (b + 1) * 256, :] = grad_ref[near, cols]
        other_ref[b * 256 : (b + 1) * 256, :] = grad_ref[far, cols].astype(BF)
    row = lax.broadcasted_iota(jnp.int32, (8, 128), 0)
    packed = jnp.zeros((8, 128), F32)
    for b in range(4):
        packed = packed + jnp.where(row == b, bias[:, b * 128 : (b + 1) * 128], 0.0)
    tail = jnp.concatenate([packed, jnp.zeros((HALF - 1032, 128), F32)], axis=0)
    mine_ref[1024:, :] = tail
    other_ref[1024:, :] = tail.astype(BF)


def piece_kernel(got_ref, out_ref):
    total = got_ref[0].astype(F32)
    for i in range(1, PIECES):
        total = total + got_ref[i].astype(F32)
    total = total.astype(BF)
    for i in range(PIECES):
        out_ref[i] = total


def final_kernel(mine_ref, other_ref, weight_ref, gain_ref, grad_ref, bias_ref, gain_grad_ref):
    core = lax.axis_index("c")
    near = pl.ds(pl.multiple_of(core * 256, 256), 256)
    far = pl.ds(pl.multiple_of((1 - core) * 256, 256), 256)
    for b in range(4):
        cols = slice(b * 128, (b + 1) * 128)
        rows = slice(b * 256, (b + 1) * 256)
        grad_ref[near, cols] = mine_ref[rows, :].astype(F32)
        grad_ref[far, cols] = other_ref[rows, :].astype(F32)
    lanes = jnp.zeros((512, 128), F32)
    for b in range(4):
        cols = slice(b * 128, (b + 1) * 128)
        lanes = lanes + grad_ref[:, cols] * weight_ref[:, cols].astype(F32)
    sums = lax.dot_general(
        jnp.ones((8, 128), F32), lanes, (((1,), (1,)), ((), ())), precision=lax.Precision.HIGHEST,
        preferred_element_type=F32,
    )
    gain_grad_ref[...] = sums[0:1, :] / gain_ref[...].astype(F32)
    tail = mine_ref[1024:1040, :].astype(F32)
    row = lax.broadcasted_iota(jnp.int32, (16, 128), 0)
    for b in range(4):
        bias_ref[:, b * 128 : (b + 1) * 128] = jnp.sum(jnp.where(row == b, tail, 0.0), axis=0, keepdims=True)


def key_sum_kernel(own_ref, a_ref, b_ref, c_ref, out0_ref, out1_ref, out2_ref, out3_ref):
    zl = lax.axis_index("zl")
    for s, out_ref in enumerate((out0_ref, out1_ref, out2_ref, out3_ref)):
        rows = pl.ds(pl.multiple_of(lax.rem(zl + s, 4) * 128, 128), 128)
        total = own_ref[rows, :] + a_ref[rows, :].astype(F32)
        total = total + b_ref[rows, :].astype(F32) + c_ref[rows, :].astype(F32)
        out_ref[...] = total.astype(out_ref.dtype)


def key_kernel(length_ref, own_ref, a_ref, b_ref, c_ref, bias_ref, out_ref):
    total = own_ref[...] + a_ref[...].astype(F32) + b_ref[...].astype(F32) + c_ref[...].astype(F32)
    total = (total + bias_ref[...].astype(F32)) * own_valid(length_ref, 128, 512)
    out_ref[...] = total.astype(BF)


def shift(value, axis, by):
    n = lax.axis_size(axis)
    return lax.ppermute(value, axis, [(i, (i + by) % n) for i in range(n)])


def on_device(text, image, offsets, counts, lengths, gain, weight, key_bias, cot):
    gain = gain.reshape(1, 512)
    own = call(mask_kernel, shape((128, 512), BF), (lengths, cot), smem=1, flops=10**6, nbytes=3 * 10**5)
    column = [own] + [shift(own, "zl", s) for s in (1, 2, 3)]
    split = call(prep_kernel, shape((16, 72, 512), BF), (text, image), flops=10**7, nbytes=5 * 10**6)
    images = lax.all_to_all(split, TP, 0, 0, tiled=True)
    column = jnp.concatenate(column, axis=0)
    got = [shift(column, "x", s) for s in (1, 2, 3)]
    normed, key0, *keys = call(
        norm_kernel,
        [shape((2048, 512), BF), shape((512, 512), F32)] + [shape((512, 512), BF)] * 3,
        (offsets, counts, text, images, weight, gain),
        smem=2,
        flops=3 * 10**9,
        nbytes=8 * 10**6,
    )
    keys = [shift(k, "x", s + 1) for s, k in enumerate(keys)]
    mine, other = call(
        grad_kernel,
        [shape((HALF, 128), F32), shape((HALF, 128), BF)],
        (normed, column, *got),
        scratch=[pltpu.VMEM((512, 512), F32)],
        flops=10**9,
        nbytes=5 * 10**6,
    )
    far = shift(other, "c", 1)
    pieces = (mine + far.astype(F32)).astype(BF).reshape(PIECES, SLAB, 128)
    pieces = lax.all_to_all(pieces, RING, 0, 0, tiled=True)
    copies = call(piece_kernel, shape((PIECES, SLAB, 128), BF), (pieces,), flops=10**6, nbytes=10**6)
    half = lax.all_to_all(copies, RING, 0, 0, tiled=True).reshape(HALF, 128)
    sums = call(
        key_sum_kernel,
        [shape((128, 512), F32)] + [shape((128, 512), BF)] * 3,
        (key0, *keys),
        flops=10**6,
        nbytes=4 * 10**6,
    )
    parts = [shift(k, "zl", s + 1) for s, k in enumerate(sums[1:])]
    key_states = call(
        key_kernel,
        shape((128, 512), BF),
        (lengths, sums[0], *parts, key_bias.reshape(1, 512)),
        smem=1,
        flops=10**6,
        nbytes=10**6,
    )
    rest = shift(half, "c", 1)
    weight_grad, bias_grad, gain_grad = call(
        final_kernel,
        [shape((512, 512), F32), shape((1, 512), F32), shape((1, 512), F32)],
        (half, rest, weight, gain),
        flops=10**7,
        nbytes=2 * 10**6,
    )
    return key_states, weight_grad, bias_grad.reshape(512), gain_grad.reshape(512)


def solution(mesh):
    fine = Mesh(mesh.devices.reshape(SIZES), AXES)
    rows = P(GRP + TP, None)
    placed = (P(GRP, TP), rows, P(GRP, None), P(GRP), P(GRP), P(TP), P(TP, None), P(), rows)
    return jax.shard_map(
        on_device,
        mesh=fine,
        in_specs=placed,
        out_specs=(rows, P(TP, None), P(), P(TP)),
        check_vma=False,
    )
```

```python
import functools

import jax
import jax.numpy as jnp
from jax import lax
from jax.experimental import pallas as pl
from jax.experimental.pallas import tpu as pltpu
from jax.sharding import Mesh
from jax.sharding import PartitionSpec as P

D = 8192
PATCH = 256
LEN = 1024
EPS = 1e-06
BF = jnp.bfloat16
F32 = jnp.float32
AXES = ("zh", "y", "c", "zl", "x")
SIZES = (3, 8, 2, 4, 4)
GRP = ("zh", "y", "c")
TP = ("zl", "x")
RING = ("zh", "y")
PIECES = 24
SLAB = 48
HALF = PIECES * SLAB
MIB = 1024 * 1024


def call(kernel, outs, args, smem=0, scratch=(), flops=0, nbytes=0, mib=50):
    in_specs = [pl.BlockSpec(memory_space=pltpu.SMEM)] * smem
    in_specs += [pl.BlockSpec(memory_space=pltpu.VMEM)] * (len(args) - smem)
    many = isinstance(outs, (list, tuple))
    vmem = pl.BlockSpec(memory_space=pltpu.VMEM)
    return pl.pallas_call(
        kernel,
        out_shape=outs,
        in_specs=in_specs,
        out_specs=[vmem] * len(outs) if many else vmem,
        scratch_shapes=list(scratch),
        cost_estimate=pl.CostEstimate(flops=flops, bytes_accessed=nbytes, transcendentals=0),
        compiler_params=pltpu.CompilerParams(vmem_limit_bytes=mib * MIB),
    )(*args)


def shape(dims, dtype):
    return jax.ShapeDtypeStruct(dims, dtype)


def own_valid(length_ref, rows, lanes):
    zl, x = lax.axis_index("zl"), lax.axis_index("x")
    position = (zl % 2) * 512 + x * 128 + lax.broadcasted_iota(jnp.int32, (rows, lanes), 0)
    return (position < length_ref[zl // 2]).astype(F32)


def mask_kernel(length_ref, cot_ref, out_ref):
    own = (cot_ref[...].astype(F32) * own_valid(length_ref, 128, 512)).astype(BF)
    for z in range(4):
        out_ref[z] = own


def prep_kernel(text_ref, image_ref, out_ref):
    rows = image_ref.shape[0]
    total = jnp.zeros((rows, 512), F32)
    for t in range(16):
        part = image_ref[:, t * 512 : (t + 1) * 512].astype(F32)
        total = total + part * part
    rstd = lax.rsqrt(jnp.sum(total, axis=1, keepdims=True) / D + EPS)
    row = lax.broadcasted_iota(jnp.int32, (8, 512), 0)
    ones = jnp.ones((8, 128), F32)
    parts = jnp.zeros((8, 512), F32)
    for j in range(4):
        lanes = jnp.zeros((512, 128), F32)
        for b in range(4):
            part = text_ref[j * 512 : (j + 1) * 512, b * 128 : (b + 1) * 128].astype(F32)
            lanes = lanes + part * part
        sums = lax.dot_general(
            ones, lanes, (((1,), (1,)), ((), ())), precision=lax.Precision.HIGHEST,
            preferred_element_type=F32,
        )
        top = sums.astype(BF).astype(F32)
        parts = parts + jnp.where(row == j, top, 0.0) + jnp.where(row == j + 4, sums - top, 0.0)
    parts = parts.astype(BF)
    for t in range(16):
        part = image_ref[:, t * 512 : (t + 1) * 512].astype(F32)
        out_ref[t, :64, :] = (part * rstd).astype(BF)
        out_ref[t, 64:, :] = parts


def block(z, q):
    return pl.ds(pl.multiple_of((z * 4 + q) * 128, 128), 128)


def norm_kernel(
    offset_ref, count_ref, text_ref, got_ref, weight_ref, gain_ref, normed_ref, key1_ref, key2_ref, key3_ref
):
    squares = jnp.concatenate([got_ref[t, 64:, :] for t in range(16)], axis=0)
    pick = lax.broadcasted_iota(jnp.int32, (128, 128), 0) % 4
    gain = gain_ref[...].astype(F32)
    for seq in range(2):
        images = jnp.concatenate([got_ref[seq * 8 + t, :64, :] for t in range(8)], axis=0)
        for part in range(4):
            base = part * 256
            ones = (pick == seq * 2 + part // 2).astype(F32).astype(BF)
            cols = slice((part % 2) * 256, (part % 2) * 256 + 256)
            total = lax.dot_general(
                squares[:, cols], ones, (((0,), (0,)), ((), ())), preferred_element_type=F32
            )
            position = base + lax.broadcasted_iota(jnp.int32, (256, 256), 0)
            column = lax.broadcasted_iota(jnp.int32, (256, 256), 1)
            narrow = base + lax.broadcasted_iota(jnp.int32, (256, 128), 0)
            hot, covered = [], None
            for slot in range(2):
                start = jnp.where(slot < count_ref[seq], offset_ref[seq, slot], LEN)
                hot.append((position - start == column).astype(F32).astype(BF))
                here = (narrow >= start) & (narrow < start + PATCH)
                covered = here if covered is None else covered | here
            scale = jnp.where(covered, 1.0, lax.rsqrt(total / D + EPS))
            placed = jnp.dot(hot[0], images[:256], preferred_element_type=F32)
            placed = placed + jnp.dot(hot[1], images[256:], preferred_element_type=F32)
            rows = slice(seq * LEN + base, seq * LEN + base + 256)
            for b in range(4):
                cols = slice(b * 128, (b + 1) * 128)
                text = text_ref[rows, cols].astype(F32)
                value = jnp.where(covered, placed[:, cols], text) * scale * gain[:, cols]
                normed_ref[rows, cols] = value.astype(BF)
    x = lax.axis_index("x")
    for s, key_ref in enumerate((key1_ref, key2_ref, key3_ref)):
        q = lax.rem(x + s + 1, 4)
        normed = jnp.concatenate([normed_ref[block(z, q), :] for z in range(4)], axis=0)
        key_ref[...] = jnp.dot(normed, weight_ref[...], preferred_element_type=F32).astype(BF)


def grad_kernel(far, normed_ref, own_ref, got1_ref, got2_ref, got3_ref, out_ref, grad_ref):
    x, core = lax.axis_index("x"), lax.axis_index("c")
    half = pl.ds(pl.multiple_of((1 - core if far else core) * 256, 256), 256)
    bias = jnp.zeros((8, 512), F32)
    for s, source in enumerate((own_ref, got1_ref, got2_ref, got3_ref)):
        q = lax.rem(x - s + 4, 4)
        normed = jnp.concatenate([normed_ref[block(z, q), half] for z in range(4)], axis=0)
        masked = source[...]
        part = lax.dot_general(normed, masked, (((0,), (0,)), ((), ())), preferred_element_type=F32)
        grad_ref[...] = part if s == 0 else grad_ref[...] + part
        bias = bias + jnp.dot(jnp.ones((8, 512), BF), masked, preferred_element_type=F32)
    row = lax.broadcasted_iota(jnp.int32, (8, 128), 0)
    packed = jnp.zeros((8, 128), F32)
    for b in range(4):
        cols = slice(b * 128, (b + 1) * 128)
        out_ref[b * 256 : (b + 1) * 256, :] = grad_ref[:, cols].astype(out_ref.dtype)
        packed = packed + jnp.where(row == b, bias[:, cols], 0.0)
    tail = jnp.concatenate([packed, jnp.zeros((HALF - 1032, 128), F32)], axis=0)
    out_ref[1024:, :] = tail.astype(out_ref.dtype)


def piece_kernel(got_ref, out_ref):
    total = got_ref[0].astype(F32)
    for i in range(1, PIECES):
        total = total + got_ref[i].astype(F32)
    total = total.astype(BF)
    for i in range(PIECES):
        out_ref[i] = total


def final_kernel(mine_ref, other_ref, weight_ref, gain_ref, grad_ref, bias_ref, gain_grad_ref):
    core = lax.axis_index("c")
    near = pl.ds(pl.multiple_of(core * 256, 256), 256)
    far = pl.ds(pl.multiple_of((1 - core) * 256, 256), 256)
    for b in range(4):
        cols = slice(b * 128, (b + 1) * 128)
        rows = slice(b * 256, (b + 1) * 256)
        grad_ref[near, cols] = mine_ref[rows, :].astype(F32)
        grad_ref[far, cols] = other_ref[rows, :].astype(F32)
    lanes = jnp.zeros((512, 128), F32)
    for b in range(4):
        cols = slice(b * 128, (b + 1) * 128)
        lanes = lanes + grad_ref[:, cols] * weight_ref[:, cols].astype(F32)
    sums = lax.dot_general(
        jnp.ones((8, 128), F32), lanes, (((1,), (1,)), ((), ())), precision=lax.Precision.HIGHEST,
        preferred_element_type=F32,
    )
    gain_grad_ref[...] = sums[0:1, :] / gain_ref[...].astype(F32)
    tail = mine_ref[1024:1040, :].astype(F32)
    row = lax.broadcasted_iota(jnp.int32, (16, 128), 0)
    for b in range(4):
        bias_ref[:, b * 128 : (b + 1) * 128] = jnp.sum(jnp.where(row == b, tail, 0.0), axis=0, keepdims=True)


def key_sum_kernel(normed_ref, weight_ref, a_ref, b_ref, c_ref, out0_ref, out1_ref, out2_ref, out3_ref):
    x, zl = lax.axis_index("x"), lax.axis_index("zl")
    for s, out_ref in enumerate((out0_ref, out1_ref, out2_ref, out3_ref)):
        z = lax.rem(zl + s, 4)
        rows = pl.ds(pl.multiple_of(z * 128, 128), 128)
        total = jnp.dot(normed_ref[block(z, x), :], weight_ref[...], preferred_element_type=F32)
        total = total + a_ref[rows, :].astype(F32) + b_ref[rows, :].astype(F32) + c_ref[rows, :].astype(F32)
        out_ref[...] = total.astype(out_ref.dtype)


def key_kernel(length_ref, own_ref, a_ref, b_ref, c_ref, bias_ref, out_ref):
    total = own_ref[...] + a_ref[...].astype(F32) + b_ref[...].astype(F32) + c_ref[...].astype(F32)
    total = (total + bias_ref[...].astype(F32)) * own_valid(length_ref, 128, 512)
    out_ref[...] = total.astype(BF)


def shift(value, axis, by):
    n = lax.axis_size(axis)
    return lax.ppermute(value, axis, [(i, (i + by) % n) for i in range(n)])


def on_device(text, image, offsets, counts, lengths, gain, weight, key_bias, cot):
    gain = gain.reshape(1, 512)
    own = call(mask_kernel, shape((4, 128, 512), BF), (lengths, cot), smem=1, flops=10**6, nbytes=10**6)
    column = lax.all_to_all(own, "zl", 0, 0, tiled=True).reshape(512, 512)
    split = call(prep_kernel, shape((16, 72, 512), BF), (text, image), flops=10**7, nbytes=5 * 10**6)
    images = lax.all_to_all(split, TP, 0, 0, tiled=True)
    got = [shift(column, "x", s) for s in (1, 2, 3)]
    normed, *keys = call(
        norm_kernel,
        [shape((2048, 512), BF)] + [shape((512, 512), BF)] * 3,
        (offsets, counts, text, images, weight, gain),
        smem=2,
        flops=3 * 10**9,
        nbytes=8 * 10**6,
    )
    ring = []
    for s, k in enumerate(keys):
        ring.append(shift(k, "x", s + 1))

    def grads(far, dtype):
        return call(
            functools.partial(grad_kernel, far),
            shape((HALF, 128), dtype),
            (normed, column, *got),
            scratch=[pltpu.VMEM((256, 512), F32)],
            flops=5 * 10**8,
            nbytes=4 * 10**6,
        )

    other = grads(True, BF)
    far = shift(other, "c", 1)
    mine = grads(False, F32)
    pieces = (mine + far.astype(F32)).astype(BF).reshape(PIECES, SLAB, 128)
    pieces = lax.all_to_all(pieces, RING, 0, 0, tiled=True)
    copies = call(piece_kernel, shape((PIECES, SLAB, 128), BF), (pieces,), flops=10**6, nbytes=10**6)
    half = lax.all_to_all(copies, RING, 0, 0, tiled=True).reshape(HALF, 128)
    sums = call(
        key_sum_kernel,
        [shape((128, 512), F32)] + [shape((128, 512), BF)] * 3,
        (normed, weight, *ring),
        flops=10**6,
        nbytes=4 * 10**6,
    )
    parts = []
    for s, k in enumerate(sums[1:]):
        parts.append(shift(k, "zl", s + 1))
    key_states = call(
        key_kernel,
        shape((128, 512), BF),
        (lengths, sums[0], *parts, key_bias.reshape(1, 512)),
        smem=1,
        flops=10**6,
        nbytes=10**6,
    )
    rest = shift(half, "c", 1)
    weight_grad, bias_grad, gain_grad = call(
        final_kernel,
        [shape((512, 512), F32), shape((1, 512), F32), shape((1, 512), F32)],
        (half, rest, weight, gain),
        flops=10**7,
        nbytes=2 * 10**6,
    )
    return key_states, weight_grad, bias_grad.reshape(512), gain_grad.reshape(512)


def solution(mesh):
    fine = Mesh(mesh.devices.reshape(SIZES), AXES)
    rows = P(GRP + TP, None)
    placed = (P(GRP, TP), rows, P(GRP, None), P(GRP), P(GRP), P(TP), P(TP, None), P(), rows)
    return jax.shard_map(
        on_device,
        mesh=fine,
        in_specs=placed,
        out_specs=(rows, P(TP, None), P(), P(TP)),
        check_vma=False,
    )
```

```python
import jax
import jax.numpy as jnp
from jax import lax
from jax.experimental import pallas as pl
from jax.experimental.pallas import tpu as pltpu
from jax.sharding import Mesh
from jax.sharding import PartitionSpec as P

D = 8192
PATCH = 256
LEN = 1024
EPS = 1e-06
BF = jnp.bfloat16
F32 = jnp.float32
AXES = ("zh", "y", "c", "zl", "x")
SIZES = (3, 8, 2, 4, 4)
GRP = ("zh", "y", "c")
TP = ("zl", "x")
RING = ("zh", "y")
PIECES = 24
SLAB = 48
HALF = PIECES * SLAB
MIB = 1024 * 1024


def call(kernel, outs, args, smem=0, scratch=(), flops=0, nbytes=0, mib=50):
    in_specs = [pl.BlockSpec(memory_space=pltpu.SMEM)] * smem
    in_specs += [pl.BlockSpec(memory_space=pltpu.VMEM)] * (len(args) - smem)
    many = isinstance(outs, (list, tuple))
    vmem = pl.BlockSpec(memory_space=pltpu.VMEM)
    return pl.pallas_call(
        kernel,
        out_shape=outs,
        in_specs=in_specs,
        out_specs=[vmem] * len(outs) if many else vmem,
        scratch_shapes=list(scratch),
        cost_estimate=pl.CostEstimate(flops=flops, bytes_accessed=nbytes, transcendentals=0),
        compiler_params=pltpu.CompilerParams(vmem_limit_bytes=mib * MIB),
    )(*args)


def shape(dims, dtype):
    return jax.ShapeDtypeStruct(dims, dtype)


def own_valid(length_ref, rows, lanes):
    zl, x = lax.axis_index("zl"), lax.axis_index("x")
    position = (zl % 2) * 512 + x * 128 + lax.broadcasted_iota(jnp.int32, (rows, lanes), 0)
    return (position < length_ref[zl // 2]).astype(F32)


def mask_kernel(length_ref, cot_ref, out_ref):
    out_ref[...] = (cot_ref[...].astype(F32) * own_valid(length_ref, 128, 512)).astype(BF)


def prep_kernel(text_ref, image_ref, out_ref):
    rows = image_ref.shape[0]
    total = jnp.zeros((rows, 512), F32)
    for t in range(16):
        part = image_ref[:, t * 512 : (t + 1) * 512].astype(F32)
        total = total + part * part
    rstd = lax.rsqrt(jnp.sum(total, axis=1, keepdims=True) / D + EPS)
    row = lax.broadcasted_iota(jnp.int32, (8, 512), 0)
    ones = jnp.ones((8, 128), F32)
    parts = jnp.zeros((8, 512), F32)
    for j in range(4):
        lanes = jnp.zeros((512, 128), F32)
        for b in range(4):
            part = text_ref[j * 512 : (j + 1) * 512, b * 128 : (b + 1) * 128].astype(F32)
            lanes = lanes + part * part
        sums = lax.dot_general(
            ones, lanes, (((1,), (1,)), ((), ())), precision=lax.Precision.HIGHEST,
            preferred_element_type=F32,
        )
        top = sums.astype(BF).astype(F32)
        parts = parts + jnp.where(row == j, top, 0.0) + jnp.where(row == j + 4, sums - top, 0.0)
    parts = parts.astype(BF)
    for t in range(16):
        part = image_ref[:, t * 512 : (t + 1) * 512].astype(F32)
        out_ref[t, :64, :] = (part * rstd).astype(BF)
        out_ref[t, 64:, :] = parts


def block(z, q):
    return pl.ds(pl.multiple_of((z * 4 + q) * 128, 128), 128)


def norm_kernel(
    offset_ref, count_ref, text_ref, got_ref, weight_ref, gain_ref, normed_ref, key1_ref, key2_ref, key3_ref
):
    squares = jnp.concatenate([got_ref[t, 64:, :] for t in range(16)], axis=0)
    pick = lax.broadcasted_iota(jnp.int32, (128, 128), 0) % 4
    gain = gain_ref[...].astype(F32)
    for seq in range(2):
        images = jnp.concatenate([got_ref[seq * 8 + t, :64, :] for t in range(8)], axis=0)
        for part in range(4):
            base = part * 256
            ones = (pick == seq * 2 + part // 2).astype(F32).astype(BF)
            cols = slice((part % 2) * 256, (part % 2) * 256 + 256)
            total = lax.dot_general(
                squares[:, cols], ones, (((0,), (0,)), ((), ())), preferred_element_type=F32
            )
            position = base + lax.broadcasted_iota(jnp.int32, (256, 256), 0)
            column = lax.broadcasted_iota(jnp.int32, (256, 256), 1)
            narrow = base + lax.broadcasted_iota(jnp.int32, (256, 128), 0)
            hot, covered = [], None
            for slot in range(2):
                start = jnp.where(slot < count_ref[seq], offset_ref[seq, slot], LEN)
                hot.append((position - start == column).astype(F32).astype(BF))
                here = (narrow >= start) & (narrow < start + PATCH)
                covered = here if covered is None else covered | here
            scale = jnp.where(covered, 1.0, lax.rsqrt(total / D + EPS))
            placed = jnp.dot(hot[0], images[:256], preferred_element_type=F32)
            placed = placed + jnp.dot(hot[1], images[256:], preferred_element_type=F32)
            rows = slice(seq * LEN + base, seq * LEN + base + 256)
            for b in range(4):
                cols = slice(b * 128, (b + 1) * 128)
                text = text_ref[rows, cols].astype(F32)
                value = jnp.where(covered, placed[:, cols], text) * scale * gain[:, cols]
                normed_ref[rows, cols] = value.astype(BF)
    x = lax.axis_index("x")
    for s, key_ref in enumerate((key1_ref, key2_ref, key3_ref)):
        q = lax.rem(x + s + 1, 4)
        normed = jnp.concatenate([normed_ref[block(z, q), :] for z in range(4)], axis=0)
        key_ref[...] = jnp.dot(normed, weight_ref[...], preferred_element_type=F32).astype(BF)


def grad_kernel(normed_ref, own_ref, got1_ref, got2_ref, got3_ref, mine_ref, other_ref, grad_ref):
    x, zl, core = lax.axis_index("x"), lax.axis_index("zl"), lax.axis_index("c")
    bias = jnp.zeros((8, 512), F32)
    for s, source in enumerate((own_ref, got1_ref, got2_ref, got3_ref)):
        q = lax.rem(x - s + 4, 4)
        normed = jnp.concatenate([normed_ref[block(lax.rem(zl - i + 4, 4), q), :] for i in range(4)], axis=0)
        masked = source[...]
        part = lax.dot_general(normed, masked, (((0,), (0,)), ((), ())), preferred_element_type=F32)
        grad_ref[...] = part if s == 0 else grad_ref[...] + part
        bias = bias + jnp.dot(jnp.ones((8, 512), BF), masked, preferred_element_type=F32)
    near = pl.ds(pl.multiple_of(core * 256, 256), 256)
    far = pl.ds(pl.multiple_of((1 - core) * 256, 256), 256)
    for b in range(4):
        cols = slice(b * 128, (b + 1) * 128)
        mine_ref[b * 256 : (b + 1) * 256, :] = grad_ref[near, cols]
        other_ref[b * 256 : (b + 1) * 256, :] = grad_ref[far, cols].astype(BF)
    row = lax.broadcasted_iota(jnp.int32, (8, 128), 0)
    packed = jnp.zeros((8, 128), F32)
    for b in range(4):
        packed = packed + jnp.where(row == b, bias[:, b * 128 : (b + 1) * 128], 0.0)
    tail = jnp.concatenate([packed, jnp.zeros((HALF - 1032, 128), F32)], axis=0)
    mine_ref[1024:, :] = tail
    other_ref[1024:, :] = tail.astype(BF)


def piece_kernel(got_ref, out_ref):
    total = got_ref[0].astype(F32)
    for i in range(1, PIECES):
        total = total + got_ref[i].astype(F32)
    total = total.astype(BF)
    for i in range(PIECES):
        out_ref[i] = total


def final_kernel(mine_ref, other_ref, weight_ref, gain_ref, grad_ref, bias_ref, gain_grad_ref):
    core = lax.axis_index("c")
    near = pl.ds(pl.multiple_of(core * 256, 256), 256)
    far = pl.ds(pl.multiple_of((1 - core) * 256, 256), 256)
    for b in range(4):
        cols = slice(b * 128, (b + 1) * 128)
        rows = slice(b * 256, (b + 1) * 256)
        grad_ref[near, cols] = mine_ref[rows, :].astype(F32)
        grad_ref[far, cols] = other_ref[rows, :].astype(F32)
    lanes = jnp.zeros((512, 128), F32)
    for b in range(4):
        cols = slice(b * 128, (b + 1) * 128)
        lanes = lanes + grad_ref[:, cols] * weight_ref[:, cols].astype(F32)
    sums = lax.dot_general(
        jnp.ones((8, 128), F32), lanes, (((1,), (1,)), ((), ())), precision=lax.Precision.HIGHEST,
        preferred_element_type=F32,
    )
    gain_grad_ref[...] = sums[0:1, :] / gain_ref[...].astype(F32)
    tail = mine_ref[1024:1040, :].astype(F32)
    row = lax.broadcasted_iota(jnp.int32, (16, 128), 0)
    for b in range(4):
        bias_ref[:, b * 128 : (b + 1) * 128] = jnp.sum(jnp.where(row == b, tail, 0.0), axis=0, keepdims=True)


def key_sum_kernel(normed_ref, weight_ref, a_ref, b_ref, c_ref, out0_ref, out1_ref, out2_ref, out3_ref):
    x, zl = lax.axis_index("x"), lax.axis_index("zl")
    for s, out_ref in enumerate((out0_ref, out1_ref, out2_ref, out3_ref)):
        z = lax.rem(zl + s, 4)
        rows = pl.ds(pl.multiple_of(z * 128, 128), 128)
        total = jnp.dot(normed_ref[block(z, x), :], weight_ref[...], preferred_element_type=F32)
        total = total + a_ref[rows, :].astype(F32) + b_ref[rows, :].astype(F32) + c_ref[rows, :].astype(F32)
        out_ref[...] = total.astype(out_ref.dtype)


def key_kernel(length_ref, own_ref, a_ref, b_ref, c_ref, bias_ref, out_ref):
    total = own_ref[...] + a_ref[...].astype(F32) + b_ref[...].astype(F32) + c_ref[...].astype(F32)
    total = (total + bias_ref[...].astype(F32)) * own_valid(length_ref, 128, 512)
    out_ref[...] = total.astype(BF)


def shift(value, axis, by):
    n = lax.axis_size(axis)
    return lax.ppermute(value, axis, [(i, (i + by) % n) for i in range(n)])


def on_device(text, image, offsets, counts, lengths, gain, weight, key_bias, cot):
    gain = gain.reshape(1, 512)
    own = call(mask_kernel, shape((128, 512), BF), (lengths, cot), smem=1, flops=10**6, nbytes=3 * 10**5)
    column = [own] + [shift(own, "zl", s) for s in (1, 2, 3)]
    split = call(prep_kernel, shape((16, 72, 512), BF), (text, image), flops=10**7, nbytes=5 * 10**6)
    images = lax.all_to_all(split, TP, 0, 0, tiled=True)
    column = jnp.concatenate(column, axis=0)
    got = [shift(column, "x", s) for s in (1, 2, 3)]
    normed, *keys = call(
        norm_kernel,
        [shape((2048, 512), BF)] + [shape((512, 512), BF)] * 3,
        (offsets, counts, text, images, weight, gain),
        smem=2,
        flops=3 * 10**9,
        nbytes=8 * 10**6,
    )
    ring = []
    for s, k in enumerate(keys):
        ring.append(shift(k, "x", s + 1))

    mine, other = call(
        grad_kernel,
        [shape((HALF, 128), F32), shape((HALF, 128), BF)],
        (normed, column, *got),
        scratch=[pltpu.VMEM((512, 512), F32)],
        flops=10**9,
        nbytes=5 * 10**6,
    )
    far = shift(other, "c", 1)
    pieces = (mine + far.astype(F32)).astype(BF).reshape(PIECES, SLAB, 128)
    pieces = lax.all_to_all(pieces, RING, 0, 0, tiled=True)
    copies = call(piece_kernel, shape((PIECES, SLAB, 128), BF), (pieces,), flops=10**6, nbytes=10**6)
    half = lax.all_to_all(copies, RING, 0, 0, tiled=True).reshape(HALF, 128)
    sums = call(
        key_sum_kernel,
        [shape((128, 512), F32)] + [shape((128, 512), BF)] * 3,
        (normed, weight, *ring),
        flops=10**6,
        nbytes=4 * 10**6,
    )
    parts = []
    for s, k in enumerate(sums[1:]):
        parts.append(shift(k, "zl", s + 1))
    key_states = call(
        key_kernel,
        shape((128, 512), BF),
        (lengths, sums[0], *parts, key_bias.reshape(1, 512)),
        smem=1,
        flops=10**6,
        nbytes=10**6,
    )
    rest = shift(half, "c", 1)
    weight_grad, bias_grad, gain_grad = call(
        final_kernel,
        [shape((512, 512), F32), shape((1, 512), F32), shape((1, 512), F32)],
        (half, rest, weight, gain),
        flops=10**7,
        nbytes=2 * 10**6,
    )
    return key_states, weight_grad, bias_grad.reshape(512), gain_grad.reshape(512)


def solution(mesh):
    fine = Mesh(mesh.devices.reshape(SIZES), AXES)
    rows = P(GRP + TP, None)
    placed = (P(GRP, TP), rows, P(GRP, None), P(GRP), P(GRP), P(TP), P(TP, None), P(), rows)
    return jax.shard_map(
        on_device,
        mesh=fine,
        in_specs=placed,
        out_specs=(rows, P(TP, None), P(), P(TP)),
        check_vma=False,
    )
```

```python
import jax
import jax.numpy as jnp
from jax import lax
from jax.experimental import pallas as pl
from jax.experimental.pallas import tpu as pltpu
from jax.sharding import Mesh
from jax.sharding import PartitionSpec as P

D = 8192
PATCH = 256
LEN = 1024
EPS = 1e-06
BF = jnp.bfloat16
F32 = jnp.float32
AXES = ("zh", "y", "c", "zl", "x")
SIZES = (3, 8, 2, 4, 4)
GRP = ("zh", "y", "c")
TP = ("zl", "x")
RING = ("zh", "y")
PIECES = 24
SLAB = 48
HALF = PIECES * SLAB
MIB = 1024 * 1024


def call(kernel, outs, args, smem=0, scratch=(), flops=0, nbytes=0, mib=50, raw=(), raw_outs=()):
    in_specs = [pl.BlockSpec(memory_space=pltpu.SMEM)] * smem
    vmem, anywhere = pl.BlockSpec(memory_space=pltpu.VMEM), pl.BlockSpec(memory_space=pl.ANY)
    in_specs += [anywhere if i in raw else vmem for i in range(smem, len(args))]
    many = isinstance(outs, (list, tuple))
    return pl.pallas_call(
        kernel,
        out_shape=outs,
        in_specs=in_specs,
        out_specs=[anywhere if i in raw_outs else vmem for i in range(len(outs))] if many else vmem,
        scratch_shapes=list(scratch),
        cost_estimate=pl.CostEstimate(flops=flops, bytes_accessed=nbytes, transcendentals=0),
        compiler_params=pltpu.CompilerParams(vmem_limit_bytes=mib * MIB),
    )(*args)


def shape(dims, dtype):
    return jax.ShapeDtypeStruct(dims, dtype)


def own_valid(length_ref, rows, lanes):
    zl, x = lax.axis_index("zl"), lax.axis_index("x")
    position = (zl % 2) * 512 + x * 128 + lax.broadcasted_iota(jnp.int32, (rows, lanes), 0)
    return (position < length_ref[zl // 2]).astype(F32)


def mask_kernel(length_ref, cot_ref, out_ref):
    out_ref[...] = (cot_ref[...].astype(F32) * own_valid(length_ref, 128, 512)).astype(BF)


def prep_kernel(text_hbm, image_hbm, out_ref, text_ref, image_ref, semaphores):
    fetched = pltpu.make_async_copy(image_hbm, image_ref, semaphores.at[4])
    fetched.start()
    texts = []
    for j in range(4):
        rows = pl.ds(j * 512, 512)
        texts.append(pltpu.make_async_copy(text_hbm.at[rows, :], text_ref.at[rows, :], semaphores.at[j]))
        texts[j].start()
    fetched.wait()
    total = jnp.zeros((64, 512), F32)
    for t in range(16):
        part = image_ref[:, t * 512 : (t + 1) * 512].astype(F32)
        total = total + part * part
    rstd = lax.rsqrt(jnp.sum(total, axis=1, keepdims=True) / D + EPS)
    for t in range(16):
        part = image_ref[:, t * 512 : (t + 1) * 512].astype(F32)
        out_ref[t, :64, :] = (part * rstd).astype(BF)
    row = lax.broadcasted_iota(jnp.int32, (8, 512), 0)
    ones = jnp.ones((8, 128), F32)
    parts = jnp.zeros((8, 512), F32)
    for j in range(4):
        lanes = jnp.zeros((512, 128), F32)
        texts[j].wait()
        for b in range(4):
            part = text_ref[j * 512 : (j + 1) * 512, b * 128 : (b + 1) * 128].astype(F32)
            lanes = lanes + part * part
        sums = lax.dot_general(
            ones, lanes, (((1,), (1,)), ((), ())), precision=lax.Precision.HIGHEST,
            preferred_element_type=F32,
        )
        top = sums.astype(BF).astype(F32)
        parts = parts + jnp.where(row == j, top, 0.0) + jnp.where(row == j + 4, sums - top, 0.0)
    parts = parts.astype(BF)
    for t in range(16):
        out_ref[t, 64:, :] = parts


def block(z, q):
    return pl.ds(pl.multiple_of((z * 4 + q) * 128, 128), 128)


def norm_kernel(
    offset_ref, count_ref, text_hbm, got_hbm, weight_ref, gain_ref, normed_hbm, key1_hbm, key2_hbm, key3_hbm,
    text_ref, got_ref, normed_ref, keys_ref, semaphores, sent,
):
    fetched = pltpu.make_async_copy(got_hbm, got_ref, semaphores.at[8])
    fetched.start()
    texts, puts = [], []
    for i in range(8):
        rows = pl.ds(i * 256, 256)
        texts.append(pltpu.make_async_copy(text_hbm.at[rows, :], text_ref.at[rows, :], semaphores.at[i]))
        texts[i].start()
        puts.append(pltpu.make_async_copy(normed_ref.at[rows, :], normed_hbm.at[rows, :], sent.at[i]))
    fetched.wait()
    squares = jnp.concatenate([got_ref[t, 64:, :] for t in range(16)], axis=0)
    pick = lax.broadcasted_iota(jnp.int32, (128, 128), 0) % 4
    gain = gain_ref[...].astype(F32)
    for seq in range(2):
        images = jnp.concatenate([got_ref[seq * 8 + t, :64, :] for t in range(8)], axis=0)
        for part in range(4):
            base = part * 256
            ones = (pick == seq * 2 + part // 2).astype(F32).astype(BF)
            cols = slice((part % 2) * 256, (part % 2) * 256 + 256)
            total = lax.dot_general(
                squares[:, cols], ones, (((0,), (0,)), ((), ())), preferred_element_type=F32
            )
            position = base + lax.broadcasted_iota(jnp.int32, (256, 256), 0)
            column = lax.broadcasted_iota(jnp.int32, (256, 256), 1)
            narrow = base + lax.broadcasted_iota(jnp.int32, (256, 128), 0)
            hot, covered = [], None
            for slot in range(2):
                start = jnp.where(slot < count_ref[seq], offset_ref[seq, slot], LEN)
                hot.append((position - start == column).astype(F32).astype(BF))
                here = (narrow >= start) & (narrow < start + PATCH)
                covered = here if covered is None else covered | here
            scale = jnp.where(covered, 1.0, lax.rsqrt(total / D + EPS))
            placed = jnp.dot(hot[0], images[:256], preferred_element_type=F32)
            placed = placed + jnp.dot(hot[1], images[256:], preferred_element_type=F32)
            rows = slice(seq * LEN + base, seq * LEN + base + 256)
            texts[seq * 4 + part].wait()
            for b in range(4):
                cols = slice(b * 128, (b + 1) * 128)
                text = text_ref[rows, cols].astype(F32)
                value = jnp.where(covered, placed[:, cols], text) * scale * gain[:, cols]
                normed_ref[rows, cols] = value.astype(BF)
            puts[seq * 4 + part].start()
    x = lax.axis_index("x")
    for s, key_hbm in enumerate((key1_hbm, key2_hbm, key3_hbm)):
        q = lax.rem(x + s + 1, 4)
        normed = jnp.concatenate([normed_ref[block(z, q), :] for z in range(4)], axis=0)
        keys_ref[s] = jnp.dot(normed, weight_ref[...], preferred_element_type=F32).astype(BF)
        puts.append(pltpu.make_async_copy(keys_ref.at[s], key_hbm, sent.at[8 + s]))
        puts[8 + s].start()
    for put in puts:
        put.wait()


def grad_kernel(
    normed_hbm, own_hbm, got1_hbm, got2_hbm, got3_hbm, mine_ref, other_ref, grad_ref, normed_ref, masked_ref, semaphores
):
    x, zl, core = lax.axis_index("x"), lax.axis_index("zl"), lax.axis_index("c")
    bias = jnp.zeros((8, 512), F32)
    copies = []
    for s, source in enumerate((own_hbm, got1_hbm, got2_hbm, got3_hbm)):
        q = lax.rem(x - s + 4, 4)
        pairs = [(source, masked_ref.at[s])]
        for i in range(4):
            rows = block(lax.rem(zl - i + 4, 4), q)
            pairs.append((normed_hbm.at[rows, :], normed_ref.at[s, pl.ds(i * 128, 128), :]))
        copies.append([pltpu.make_async_copy(a, b, semaphores.at[s, i]) for i, (a, b) in enumerate(pairs)])
        for copy in copies[s]:
            copy.start()
    for s in range(4):
        for copy in copies[s]:
            copy.wait()
        normed, masked = normed_ref[s], masked_ref[s]
        part = lax.dot_general(normed, masked, (((0,), (0,)), ((), ())), preferred_element_type=F32)
        grad_ref[...] = part if s == 0 else grad_ref[...] + part
        bias = bias + jnp.dot(jnp.ones((8, 512), BF), masked, preferred_element_type=F32)
    near = pl.ds(pl.multiple_of(core * 256, 256), 256)
    far = pl.ds(pl.multiple_of((1 - core) * 256, 256), 256)
    for b in range(4):
        cols = slice(b * 128, (b + 1) * 128)
        mine_ref[b * 256 : (b + 1) * 256, :] = grad_ref[near, cols]
        other_ref[b * 256 : (b + 1) * 256, :] = grad_ref[far, cols].astype(BF)
    row = lax.broadcasted_iota(jnp.int32, (8, 128), 0)
    packed = jnp.zeros((8, 128), F32)
    for b in range(4):
        packed = packed + jnp.where(row == b, bias[:, b * 128 : (b + 1) * 128], 0.0)
    tail = jnp.concatenate([packed, jnp.zeros((HALF - 1032, 128), F32)], axis=0)
    mine_ref[1024:, :] = tail
    other_ref[1024:, :] = tail.astype(BF)


def piece_kernel(got_ref, out_ref):
    total = got_ref[0].astype(F32)
    for i in range(1, PIECES):
        total = total + got_ref[i].astype(F32)
    total = total.astype(BF)
    for i in range(PIECES):
        out_ref[i] = total


def final_kernel(mine_ref, other_ref, weight_ref, gain_ref, grad_ref, bias_ref, gain_grad_ref):
    core = lax.axis_index("c")
    near = pl.ds(pl.multiple_of(core * 256, 256), 256)
    far = pl.ds(pl.multiple_of((1 - core) * 256, 256), 256)
    for b in range(4):
        cols = slice(b * 128, (b + 1) * 128)
        rows = slice(b * 256, (b + 1) * 256)
        grad_ref[near, cols] = mine_ref[rows, :].astype(F32)
        grad_ref[far, cols] = other_ref[rows, :].astype(F32)
    lanes = jnp.zeros((512, 128), F32)
    for b in range(4):
        cols = slice(b * 128, (b + 1) * 128)
        lanes = lanes + grad_ref[:, cols] * weight_ref[:, cols].astype(F32)
    sums = lax.dot_general(
        jnp.ones((8, 128), F32), lanes, (((1,), (1,)), ((), ())), precision=lax.Precision.HIGHEST,
        preferred_element_type=F32,
    )
    gain_grad_ref[...] = sums[0:1, :] / gain_ref[...].astype(F32)
    tail = mine_ref[1024:1040, :].astype(F32)
    row = lax.broadcasted_iota(jnp.int32, (16, 128), 0)
    for b in range(4):
        bias_ref[:, b * 128 : (b + 1) * 128] = jnp.sum(jnp.where(row == b, tail, 0.0), axis=0, keepdims=True)


def key_sum_kernel(normed_ref, weight_ref, a_ref, b_ref, c_ref, out0_ref, out1_ref, out2_ref, out3_ref):
    x, zl = lax.axis_index("x"), lax.axis_index("zl")
    for s, out_ref in enumerate((out0_ref, out1_ref, out2_ref, out3_ref)):
        z = lax.rem(zl + s, 4)
        rows = pl.ds(pl.multiple_of(z * 128, 128), 128)
        total = jnp.dot(normed_ref[block(z, x), :], weight_ref[...], preferred_element_type=F32)
        total = total + a_ref[rows, :].astype(F32) + b_ref[rows, :].astype(F32) + c_ref[rows, :].astype(F32)
        out_ref[...] = total.astype(out_ref.dtype)


def key_kernel(length_ref, own_ref, a_ref, b_ref, c_ref, bias_ref, out_ref):
    total = own_ref[...] + a_ref[...].astype(F32) + b_ref[...].astype(F32) + c_ref[...].astype(F32)
    total = (total + bias_ref[...].astype(F32)) * own_valid(length_ref, 128, 512)
    out_ref[...] = total.astype(BF)


def shift(value, axis, by):
    n = lax.axis_size(axis)
    return lax.ppermute(value, axis, [(i, (i + by) % n) for i in range(n)])


def on_device(text, image, offsets, counts, lengths, gain, weight, key_bias, cot):
    gain = gain.reshape(1, 512)
    own = call(mask_kernel, shape((128, 512), BF), (lengths, cot), smem=1, flops=10**6, nbytes=3 * 10**5)
    column = [own] + [shift(own, "zl", s) for s in (1, 2, 3)]
    split = call(
        prep_kernel,
        shape((16, 72, 512), BF),
        (text, image),
        scratch=[pltpu.VMEM((2048, 512), BF), pltpu.VMEM((64, 8192), BF), pltpu.SemaphoreType.DMA((5,))],
        flops=10**7,
        nbytes=5 * 10**6,
        mib=56,
        raw=(0, 1),
    )
    images = lax.all_to_all(split, TP, 0, 0, tiled=True)
    column = jnp.concatenate(column, axis=0)
    got = [shift(column, "x", s) for s in (1, 2, 3)]
    normed, *keys = call(
        norm_kernel,
        [shape((2048, 512), BF)] + [shape((512, 512), BF)] * 3,
        (offsets, counts, text, images, weight, gain),
        smem=2,
        scratch=[
            pltpu.VMEM((2048, 512), BF),
            pltpu.VMEM((16, 72, 512), BF),
            pltpu.VMEM((2048, 512), BF),
            pltpu.VMEM((3, 512, 512), BF),
            pltpu.SemaphoreType.DMA((9,)),
            pltpu.SemaphoreType.DMA((11,)),
        ],
        raw=(2, 3),
        raw_outs=(0, 1, 2, 3),
        flops=3 * 10**9,
        nbytes=8 * 10**6,
    )
    ring = []
    for s, k in enumerate(keys):
        ring.append(shift(k, "x", s + 1))

    mine, other = call(
        grad_kernel,
        [shape((HALF, 128), F32), shape((HALF, 128), BF)],
        (normed, column, *got),
        scratch=[
            pltpu.VMEM((512, 512), F32),
            pltpu.VMEM((4, 512, 512), BF),
            pltpu.VMEM((4, 512, 512), BF),
            pltpu.SemaphoreType.DMA((4, 5)),
        ],
        raw=(0, 1, 2, 3, 4),
        flops=10**9,
        nbytes=5 * 10**6,
    )
    far = shift(other, "c", 1)
    pieces = (mine + far.astype(F32)).astype(BF).reshape(PIECES, SLAB, 128)
    pieces = lax.all_to_all(pieces, RING, 0, 0, tiled=True)
    copies = call(piece_kernel, shape((PIECES, SLAB, 128), BF), (pieces,), flops=10**6, nbytes=10**6)
    half = lax.all_to_all(copies, RING, 0, 0, tiled=True).reshape(HALF, 128)
    sums = call(
        key_sum_kernel,
        [shape((128, 512), F32)] + [shape((128, 512), BF)] * 3,
        (normed, weight, *ring),
        flops=10**6,
        nbytes=4 * 10**6,
    )
    parts = []
    for s, k in enumerate(sums[1:]):
        parts.append(shift(k, "zl", s + 1))
    key_states = call(
        key_kernel,
        shape((128, 512), BF),
        (lengths, sums[0], *parts, key_bias.reshape(1, 512)),
        smem=1,
        flops=10**6,
        nbytes=10**6,
    )
    rest = shift(half, "c", 1)
    weight_grad, bias_grad, gain_grad = call(
        final_kernel,
        [shape((512, 512), F32), shape((1, 512), F32), shape((1, 512), F32)],
        (half, rest, weight, gain),
        flops=10**7,
        nbytes=2 * 10**6,
    )
    return key_states, weight_grad, bias_grad.reshape(512), gain_grad.reshape(512)


def solution(mesh):
    fine = Mesh(mesh.devices.reshape(SIZES), AXES)
    rows = P(GRP + TP, None)
    placed = (P(GRP, TP), rows, P(GRP, None), P(GRP), P(GRP), P(TP), P(TP, None), P(), rows)
    return jax.shard_map(
        on_device,
        mesh=fine,
        in_specs=placed,
        out_specs=(rows, P(TP, None), P(), P(TP)),
        check_vma=False,
    )
```
